32 devices in a mesh: slab: 8 (over z, core), grp: 4 (over y, x).
Axes of the slice: x: 2, y: 2, z: 4, core: 2. Of those that a mesh axis runs over, the one named last changes fastest.
Arguments:
- comp: float32 [256, 128, 128], P(('slab', 'grp')), may hold values from -1 to 1
- guess: float32 [64, 32, 32], P('slab', 'grp'), may hold values from -3 to 3
Outputs:
- comp_next: float32 [256, 128, 128], P(('slab', 'grp'))
- potential: float32 [64, 32, 32], P('slab', 'grp')
The draws below stay inside these ranges and needn't reach their ends.
All inputs are finite; a program needn't handle non-finite values.
Results may differ from the reference program's by a relative error of at most 0.00002.
Values sent between devices are 32-bit elements; how exact they have to be, the bound alone decides.
No kernel may reach another device: no remote copies, remote signals or barrier semaphores. Data moves between devices by JAX's collectives and lax.ppermute only.
A program may use at most 64 MiB of HBM per device.

```python
import jax
import jax.numpy as jnp

NY = 128
NZ = 128
NPRE = 1
NCOARSE = 3
NPOST = 2
NX = 256
CNX = 64
CNY = 32
CNZ = 32


def level_of(key, shape, split, low, largest):
    level = 1.0
    for dim, shards_of in split:
        steps = jax.random.uniform(jax.random.fold_in(jax.random.fold_in(key, 6), dim), (shards_of,), jnp.float32, low / len(split), largest / len(split))
        level = level * jnp.repeat(jnp.exp(steps), shape[dim] // shards_of).reshape((-1,) + (1,) * (len(shape) - 1 - dim))
    return level


def gaussian(rng, dims, deviation, limit, shards=(), kind=jnp.bfloat16):
    values = deviation * jax.random.normal(rng, dims, jnp.float32)
    if shards:
        values = values * level_of(rng, dims, shards, -0.22, 0.18)
    return jnp.clip(values, -limit, limit).astype(kind)


def setup_inputs(seed: int = 0) -> dict:
    key_list = jax.random.split(jax.random.key(seed), 3)
    comp = jnp.clip(jax.random.uniform(key_list[0], (NX, NY, NZ), jnp.float32, -1.0, 1.0) * level_of(key_list[0], (NX, NY, NZ), ((0, 32),), -0.4, 0.0), -1.0, 1.0)
    guess = gaussian(key_list[1], (CNX, CNY, CNZ), 0.5, 3.0, ((0, 8), (1, 4)), jnp.float32)
    return {"comp": comp, "guess": guess}


gradient_energy = 0.5
screening = 0.5
damping = 0.8
long_range = 4.0
time_step = 0.02


def laplace_padded(padded):
    inner = padded[1:-1, 1:-1, 1:-1]
    beside_all = padded[2:, 1:-1, 1:-1] + padded[:-2, 1:-1, 1:-1]
    beside_all = beside_all + padded[1:-1, 2:, 1:-1] + padded[1:-1, :-2, 1:-1]
    beside_all = beside_all + padded[1:-1, 1:-1, 2:] + padded[1:-1, 1:-1, :-2]
    return beside_all - 6.0 * inner


def laplace(field):
    return laplace_padded(jnp.pad(field, 1))


def block_mean(field, factor):
    first, second, third = field.shape
    return field.reshape(first // factor, factor, second // factor, factor, third // factor, factor).mean(axis=(1, 3, 5))


def expand(field, factor):
    first, second, third = field.shape
    wide = jnp.broadcast_to(field[:, None, :, None, :, None], (first, factor, second, factor, third, factor))
    return wide.reshape(first * factor, second * factor, third * factor)


def smooth(potential, source):
    operated = screening * potential - laplace(potential)
    return potential + damping * (source - operated) / (screening + 6.0)


def reference(comp, guess):
    chem = comp * comp * comp - comp - gradient_energy * laplace(comp)
    source = block_mean(comp, 4)
    potential = guess
    for sweep in range(NPRE):
        potential = smooth(potential, source)
    residual = source - (screening * potential - laplace(potential))
    coarsest = block_mean(residual, 2)
    correction = damping * coarsest / (screening + 1.5)
    for sweep in range(NCOARSE - 1):
        operated = screening * correction - 0.25 * laplace(correction)
        correction = correction + damping * (coarsest - operated) / (screening + 1.5)
    potential = potential + expand(correction, 2)
    for sweep in range(NPOST):
        potential = smooth(potential, source)
    field = chem + long_range * expand(potential, 4)
    comp_next = comp + time_step * laplace(field)
    return comp_next, potential
```

```python
import functools

import jax
import jax.numpy as jnp
from jax import lax
from jax.experimental import pallas as pl
from jax.experimental.pallas import tpu as pltpu
from jax.sharding import PartitionSpec as P

NPRE = 1
NCOARSE = 3
NPOST = 2

gradient_energy = 0.5
screening = 0.5
damping = 0.8
long_range = 4.0
time_step = 0.02

LANES = 128
QUAD = 4
HALO = 3

VMEM = pl.BlockSpec(memory_space=pltpu.VMEM)


def lanes_of(shape):
    return lax.broadcasted_iota(jnp.int32, shape, len(shape) - 1)


def rows_of(shape):
    return lax.broadcasted_iota(jnp.int32, shape, len(shape) - 2)


def exact_dot(a, b):
    return jnp.dot(a, b, preferred_element_type=jnp.float32, precision=lax.Precision.HIGHEST)


def pack_kernel(comp_ref, guess_ref, message_ref, first_ref, second_ref):
    columns = guess_ref.shape[2]
    rows = comp_ref.shape[1] // 4
    half = rows // 2
    pooled = []
    for plane in range(comp_ref.shape[0] // 4):
        total = None
        for i in range(4):
            for j in range(4):
                part = comp_ref[4 * plane + i, pl.ds(j, rows, stride=4), :]
                total = part if total is None else total + part
        pooled.append(total)
    stacked = jnp.concatenate(
        [pooled[0][:half], pooled[1][:half], pooled[0][half:], pooled[1][half:]], axis=0
    )
    square = (comp_ref.shape[2], LANES)
    pool = jnp.where(rows_of(square) // 4 == lanes_of(square) % columns, 1.0 / 64.0, 0.0)
    spread = exact_dot(stacked, pool.astype(jnp.float32))
    where = lanes_of((half, LANES)) // columns
    packed = spread[:half]
    for block in range(1, QUAD):
        packed = jnp.where(where == block, spread[block * half : (block + 1) * half], packed)
    message_ref[0:half, :] = packed
    planes, block_rows = guess_ref.shape[0], guess_ref.shape[1]
    for quad in range(planes // QUAD):
        at = half + quad * block_rows
        for i in range(QUAD):
            message_ref[at : at + block_rows, i * columns : (i + 1) * columns] = guess_ref[
                QUAD * quad + i
            ]
    odd = lax.rem(lax.axis_index("grp"), 2)
    top = comp_ref.shape[0] - 2
    first_ref[...] = comp_ref[pl.ds(top * (1 - odd), 2)]
    second_ref[...] = comp_ref[pl.ds(top * odd, 2)]


def pack(comp, guess):
    outer = jax.ShapeDtypeStruct((2,) + comp.shape[1:], jnp.float32)
    message = jax.ShapeDtypeStruct((32, LANES), jnp.float32)
    return pl.pallas_call(
        pack_kernel,
        out_shape=(message, outer, outer),
        in_specs=[VMEM] * 2,
        out_specs=(VMEM,) * 3,
        cost_estimate=pl.CostEstimate(flops=2_000_000, bytes_accessed=800_000, transcendentals=0),
        name="pack",
    )(comp, guess)


def beside_in_plane(v):
    rows, lanes = rows_of(v.shape), lanes_of(v.shape)
    last_row, last_lane = v.shape[0] - 1, v.shape[1] - 1
    total = jnp.where(rows == 0, 0.0, pltpu.roll(v, 1, 0))
    total = total + jnp.where(rows == last_row, 0.0, pltpu.roll(v, last_row, 0))
    total = total + jnp.where(lanes == 0, 0.0, pltpu.roll(v, 1, 1))
    return total + jnp.where(lanes == last_lane, 0.0, pltpu.roll(v, last_lane, 1))


def base_kernel(comp_ref, first_ref, second_ref, base_ref, chem_ref):
    planes = comp_ref.shape[0]
    group, groups = lax.axis_index("grp"), lax.axis_size("grp")
    index = lax.axis_index("slab") * groups + group
    devices = lax.axis_size("slab") * groups
    odd = lax.rem(group, 2) == 1

    def plane(f):
        if f < 0:
            return jnp.where(odd, first_ref[f + 2], second_ref[f + 2])
        if f >= planes:
            return jnp.where(odd, second_ref[f - planes], first_ref[f - planes])
        return comp_ref[f]

    for f in range(-1, planes + 1):
        c = plane(f)
        beside = beside_in_plane(c) + plane(f - 1) + plane(f + 1)
        chem = c * c * c - c - gradient_energy * (beside - 6.0 * c)
        if f < 0:
            chem = jnp.where(index > 0, chem, 0.0)
        if f >= planes:
            chem = jnp.where(index < devices - 1, chem, 0.0)
        chem_ref[f + 1] = chem
    for f in range(planes):
        v = chem_ref[f + 1]
        beside = beside_in_plane(v) + chem_ref[f] + chem_ref[f + 2]
        base_ref[f] = comp_ref[f] + time_step * (beside - 6.0 * v)


def base_of(comp, first, second):
    return pl.pallas_call(
        base_kernel,
        out_shape=jax.ShapeDtypeStruct(comp.shape, jnp.float32),
        in_specs=[VMEM] * 3,
        out_specs=VMEM,
        scratch_shapes=[pltpu.VMEM((comp.shape[0] + 2,) + comp.shape[1:], jnp.float32)],
        cost_estimate=pl.CostEstimate(flops=6_000_000, bytes_accessed=1_500_000, transcendentals=0),
        name="base",
    )(comp, first, second)


def along(v, quad, step):
    shift = (-32 * step) % LANES
    here = pltpu.roll(v[quad], shift, 1)
    other = quad + (1 if step > 0 else -1)
    lanes = lanes_of(here.shape)
    own = lanes < LANES - 32 * step if step > 0 else lanes >= -32 * step
    if 0 <= other < len(v):
        return jnp.where(own, here, pltpu.roll(v[other], shift, 1))
    return jnp.where(own, here, 0.0)


def beside(v, quad, step):
    here = v[quad]
    rows, columns = rows_of(here.shape), lanes_of(here.shape) % 32
    total = along(v, quad, step) + along(v, quad, -step)
    total = total + jnp.where(rows < step, 0.0, pltpu.roll(here, step, 0))
    total = total + jnp.where(rows >= 32 - step, 0.0, pltpu.roll(here, 32 - step, 0))
    total = total + jnp.where(columns < step, 0.0, pltpu.roll(here, step, 1))
    return total + jnp.where(columns >= 32 - step, 0.0, pltpu.roll(here, LANES - step, 1))


def operated(v, quad):
    return screening * v[quad] - (beside(v, quad, 1) - 6.0 * v[quad])


def cell_mean(v):
    rows, lanes = rows_of(v.shape), lanes_of(v.shape)
    v = v + jnp.where(lanes % 2 == 0, pltpu.roll(v, LANES - 1, 1), pltpu.roll(v, 1, 1))
    v = v + jnp.where(
        (lanes // 32) % 2 == 0, pltpu.roll(v, LANES - 32, 1), pltpu.roll(v, 32, 1)
    )
    v = v + jnp.where(rows % 2 == 0, pltpu.roll(v, 31, 0), pltpu.roll(v, 1, 0))
    return v * 0.125


def cycle_kernel(edged, *refs):
    base_ref, own_ref, core_ref, chip_ref = refs[:4]
    refs = refs[4:]
    if edged:
        edge_ref, refs = refs[0], refs[1:]
    next_ref, potential_ref, guess_s, window_s = refs
    groups = lax.axis_size("grp")
    slab, slabs, group = lax.axis_index("slab"), lax.axis_size("slab"), lax.axis_index("grp")
    quads = groups // 2
    block = 32 // groups
    low_half = lanes_of((16, LANES)) < 64
    odd = lax.rem(slab, 2) == 1

    def low(*at):
        return jnp.where(odd, core_ref[at], chip_ref[at])

    def high(*at):
        return jnp.where(odd, chip_ref[at], core_ref[at])

    def own(*at):
        return own_ref[at]

    def source_of(even, uneven):
        top = jnp.where(low_half, even, pltpu.roll(uneven, 64, 1))
        bottom = jnp.where(low_half, pltpu.roll(even, 64, 1), uneven)
        return jnp.concatenate([top, bottom], axis=0)

    source, count = [], 0

    def take(read, quad):
        nonlocal count
        source.append(source_of(read(2 * quad, pl.ds(0, 16)), read(2 * quad + 1, pl.ds(0, 16))))
        for g in range(groups):
            guess_s[count, g * block : (g + 1) * block] = read(
                g, pl.ds(16 + quad * block, block)
            )
        count += 1

    def take_edge():
        nonlocal count
        source.append(source_of(edge_ref[0:16], edge_ref[16:32]))
        guess_s[count] = edge_ref[32:64]
        count += 1

    near = HALO - 1 if edged else HALO
    if edged:
        take_edge()
    for quad in range(quads - near, quads):
        take(low, quad)
    for quad in range(quads):
        take(own, quad)
    for quad in range(near):
        take(high, quad)
    if edged:
        take_edge()
    total = quads + 2 * HALO

    inside = []
    for quad in range(total):
        away = quad - HALO
        if away < 0:
            reach = -(away // quads)
            inside.append(jnp.where(slab >= reach, 1.0, 0.0))
        elif away >= quads:
            inside.append(jnp.where(slab + away // quads < slabs, 1.0, 0.0))
        else:
            inside.append(None)

    def kept(v, quad):
        return v if inside[quad] is None else v * inside[quad]

    guess = [guess_s[quad] for quad in range(total)]
    scale = damping / (screening + 6.0)
    pre = [
        kept(guess[quad] + scale * (source[quad] - operated(guess, quad)), quad)
        for quad in range(total)
    ]
    coarsest = [
        kept(cell_mean(source[quad] - operated(pre, quad)), quad) for quad in range(1, total - 1)
    ]
    scale_b = damping / (screening + 1.5)
    correction = [scale_b * v for v in coarsest]
    for sweep in range(NCOARSE - 1):
        last = sweep == NCOARSE - 2
        updated = []
        for quad in range(len(correction)):
            if last and quad in (0, len(correction) - 1):
                updated.append(None)
                continue
            c = correction[quad]
            applied = screening * c - 0.25 * (beside(correction, quad, 2) - 6.0 * c)
            updated.append(kept(c + scale_b * (coarsest[quad] - applied), quad + 1))
        correction = updated
    found = [pre[quad] + correction[quad - 1] for quad in range(2, total - 2)]
    for sweep in range(NPOST):
        found = [
            kept(v + scale * (source[quad + 2] - operated(found, quad)), quad + 2)
            for quad, v in enumerate(found)
        ]

    for quad in range(len(found)):
        window_s[quad] = found[quad]
    for quad in range(quads):
        rows = window_s[quad + 1, pl.ds(pl.multiple_of(group * block, block), block), :]
        for i in range(QUAD):
            potential_ref[QUAD * quad + i] = rows[:, 32 * i : 32 * (i + 1)]

    picked = []
    for i in range(4):
        at = 2 * group + 3 + i
        picked.append(
            pltpu.roll(window_s[at // QUAD], lax.rem(LANES - 32 * lax.rem(at, QUAD), LANES), 1)
        )
    square = (LANES, LANES)
    widen = jnp.where(rows_of(square) == lanes_of(square) // 4, 1.0, 0.0).astype(jnp.float32)
    wide = exact_dot(jnp.concatenate(picked, axis=0), widen)
    wide = [wide[32 * i : 32 * (i + 1)] for i in range(4)]
    factor = time_step * long_range
    rows, lanes = rows_of((32, LANES)), lanes_of((32, LANES))
    for coarse in range(2):
        here = wide[coarse + 1]
        across = jnp.where(lanes == 0, 0.0, pltpu.roll(here, 1, 1))
        across = across + jnp.where(lanes == LANES - 1, 0.0, pltpu.roll(here, LANES - 1, 1))
        middle = factor * (across - 2.0 * here)
        before = middle + factor * (jnp.where(rows == 0, 0.0, pltpu.roll(here, 1, 0)) - here)
        after = middle + factor * (jnp.where(rows == 31, 0.0, pltpu.roll(here, 31, 0)) - here)
        down = factor * (wide[coarse] - here)
        up = factor * (wide[coarse + 2] - here)
        for f in range(4):
            for j in range(4):
                term = (before, middle, middle, after)[j]
                if f == 0:
                    term = term + down
                if f == 3:
                    term = term + up
                at = (4 * coarse + f, pl.ds(j, 32, stride=4), slice(None))
                next_ref[at] = base_ref[at] + term


def cycle(base, own, core, chip, edge, guess):
    groups = own.shape[0]
    total = groups // 2 + 2 * HALO
    operands = [base, own, core, chip] + ([] if edge is None else [edge])
    return pl.pallas_call(
        functools.partial(cycle_kernel, edge is not None),
        out_shape=(
            jax.ShapeDtypeStruct(base.shape, jnp.float32),
            jax.ShapeDtypeStruct(guess.shape, jnp.float32),
        ),
        in_specs=[VMEM] * len(operands),
        out_specs=(VMEM, VMEM),
        scratch_shapes=[
            pltpu.VMEM((total, 32, LANES), jnp.float32),
            pltpu.VMEM((total - 4, 32, LANES), jnp.float32),
        ],
        cost_estimate=pl.CostEstimate(flops=6_000_000, bytes_accessed=1_500_000, transcendentals=0),
        name="cycle",
    )(*operands)


def per_device(comp, guess):
    slabs, groups = lax.axis_size("slab"), lax.axis_size("grp")
    group = lax.axis_index("grp")
    both = ("slab", "grp")
    devices = slabs * groups
    quads = groups // 2

    message, first, second = pack(comp, guess)

    bundle = jnp.zeros((groups,) + message.shape, jnp.float32)
    bundle = lax.dynamic_update_slice(bundle, message[None], (group, 0, 0))
    received = [
        lax.ppermute(message, "grp", [(i, i ^ k) for i in range(groups)]) for k in range(1, groups)
    ]
    for k, block in enumerate(received, 1):
        bundle = lax.dynamic_update_slice(bundle, block[None], (group ^ k, 0, 0))

    first = lax.ppermute(first, both, [(d, d ^ 1) for d in range(devices)])
    second = lax.ppermute(
        second, both, [p for d in range(1, devices - 1, 2) for p in ((d, d + 1), (d + 1, d))]
    )

    core = lax.ppermute(bundle, "slab", [(i, i ^ 1) for i in range(slabs)])
    chip = lax.ppermute(
        bundle, "slab", [p for i in range(1, slabs - 1, 2) for p in ((i, i + 1), (i + 1, i))]
    )
    edge = None
    if quads < HALO:
        block = 32 // groups
        is_first = group == 0
        edge = jnp.concatenate(
            [
                jnp.where(is_first, bundle[groups - 2 :, :16], bundle[:2, :16]).reshape(32, LANES),
                jnp.where(
                    is_first,
                    bundle[:, 16 + (quads - 1) * block : 16 + quads * block],
                    bundle[:, 16 : 16 + block],
                ).reshape(32, LANES),
            ],
            axis=0,
        )
        pairs = []
        for i in range(slabs - 2):
            pairs.append((i * groups, (i + 2) * groups))
            pairs.append(((i + 2) * groups + groups - 1, i * groups + groups - 1))
        edge = lax.ppermute(edge, both, pairs)

    base = base_of(comp, first, second)
    return cycle(base, bundle, core, chip, edge, guess)


def solution(mesh):
    placed = (P(("slab", "grp"), None, None), P("slab", "grp", None))
    return jax.shard_map(
        per_device,
        mesh=mesh,
        in_specs=placed,
        out_specs=placed,
        check_vma=False,
    )
```

```python
import functools

import jax
import jax.numpy as jnp
from jax import lax
from jax.experimental import pallas as pl
from jax.experimental.pallas import tpu as pltpu
from jax.sharding import PartitionSpec as P

NCOARSE = 3
NPOST = 2

gradient_energy = 0.5
screening = 0.5
damping = 0.8
long_range = 4.0
time_step = 0.02

LANES = 128
QUAD = 4
HALO = 3

VMEM = pl.BlockSpec(memory_space=pltpu.VMEM)
PARAMS = pltpu.CompilerParams(vmem_limit_bytes=8 * 2**20)


def lanes_of(shape):
    return lax.broadcasted_iota(jnp.int32, shape, len(shape) - 1)


def rows_of(shape):
    return lax.broadcasted_iota(jnp.int32, shape, len(shape) - 2)


def exact_dot(a, b):
    return jnp.dot(a, b, preferred_element_type=jnp.float32, precision=lax.Precision.HIGHEST)


def pack_guess_kernel(guess_ref, packed_ref):
    planes, rows, columns = guess_ref.shape
    for quad in range(planes // QUAD):
        at = quad * rows
        for i in range(QUAD):
            packed_ref[at : at + rows, i * columns : (i + 1) * columns] = guess_ref[QUAD * quad + i]


def pack_guess(guess):
    return pl.pallas_call(
        pack_guess_kernel,
        out_shape=jax.ShapeDtypeStruct((16, LANES), jnp.float32),
        in_specs=[VMEM],
        out_specs=VMEM,
        cost_estimate=pl.CostEstimate(flops=10_000, bytes_accessed=40_000, transcendentals=0),
        compiler_params=PARAMS,
        name="pack_guess",
    )(guess)


def pack_kernel(comp_ref, guess_ref, message_ref, first_ref, second_ref):
    columns = 32
    rows = comp_ref.shape[1] // 4
    half = rows // 2
    message_ref[half:, :] = guess_ref[...]
    pooled = []
    for plane in range(comp_ref.shape[0] // 4):
        total = None
        for i in range(4):
            for j in range(4):
                part = comp_ref[4 * plane + i, pl.ds(j, rows, stride=4), :]
                total = part if total is None else total + part
        pooled.append(total)
    stacked = jnp.concatenate(
        [pooled[0][:half], pooled[1][:half], pooled[0][half:], pooled[1][half:]], axis=0
    )
    square = (comp_ref.shape[2], LANES)
    pool = jnp.where(rows_of(square) // 4 == lanes_of(square) % columns, 1.0 / 64.0, 0.0)
    spread = exact_dot(stacked, pool.astype(jnp.float32))
    where = lanes_of((half, LANES)) // columns
    packed = spread[:half]
    for block in range(1, QUAD):
        packed = jnp.where(where == block, spread[block * half : (block + 1) * half], packed)
    message_ref[0:half, :] = packed
    odd = lax.rem(lax.axis_index("grp"), 2)
    top = comp_ref.shape[0] - 2
    first_ref[...] = comp_ref[pl.ds(top * (1 - odd), 2)]
    second_ref[...] = comp_ref[pl.ds(top * odd, 2)]


def pack(comp, guess):
    outer = jax.ShapeDtypeStruct((2,) + comp.shape[1:], jnp.float32)
    message = jax.ShapeDtypeStruct((32, LANES), jnp.float32)
    return pl.pallas_call(
        pack_kernel,
        out_shape=(message, outer, outer),
        in_specs=[VMEM] * 2,
        out_specs=(VMEM,) * 3,
        cost_estimate=pl.CostEstimate(flops=2_000_000, bytes_accessed=800_000, transcendentals=0),
        compiler_params=PARAMS,
        name="pack",
    )(comp, pack_guess(guess))


def beside_in_plane(v):
    rows, lanes = rows_of(v.shape), lanes_of(v.shape)
    last_row, last_lane = v.shape[0] - 1, v.shape[1] - 1
    total = jnp.where(rows == 0, 0.0, pltpu.roll(v, 1, 0))
    total = total + jnp.where(rows == last_row, 0.0, pltpu.roll(v, last_row, 0))
    total = total + jnp.where(lanes == 0, 0.0, pltpu.roll(v, 1, 1))
    return total + jnp.where(lanes == last_lane, 0.0, pltpu.roll(v, last_lane, 1))


def base_kernel(comp_ref, first_ref, second_ref, base_ref, chem_ref):
    planes = comp_ref.shape[0]
    group, groups = lax.axis_index("grp"), lax.axis_size("grp")
    index = lax.axis_index("slab") * groups + group
    devices = lax.axis_size("slab") * groups
    odd = lax.rem(group, 2) == 1

    def plane(f):
        if f < 0:
            return jnp.where(odd, first_ref[f + 2], second_ref[f + 2])
        if f >= planes:
            return jnp.where(odd, second_ref[f - planes], first_ref[f - planes])
        return comp_ref[f]

    for f in range(-1, planes + 1):
        c = plane(f)
        beside = beside_in_plane(c) + plane(f - 1) + plane(f + 1)
        chem = c * c * c - c - gradient_energy * (beside - 6.0 * c)
        if f < 0:
            chem = jnp.where(index > 0, chem, 0.0)
        if f >= planes:
            chem = jnp.where(index < devices - 1, chem, 0.0)
        chem_ref[f + 1] = chem
    for f in range(planes):
        v = chem_ref[f + 1]
        beside = beside_in_plane(v) + chem_ref[f] + chem_ref[f + 2]
        base_ref[f] = comp_ref[f] + time_step * (beside - 6.0 * v)


def base_of(comp, first, second):
    return pl.pallas_call(
        base_kernel,
        out_shape=jax.ShapeDtypeStruct(comp.shape, jnp.float32),
        in_specs=[VMEM] * 3,
        out_specs=VMEM,
        scratch_shapes=[pltpu.VMEM((comp.shape[0] + 2,) + comp.shape[1:], jnp.float32)],
        cost_estimate=pl.CostEstimate(flops=6_000_000, bytes_accessed=1_500_000, transcendentals=0),
        compiler_params=PARAMS,
        name="base",
    )(comp, first, second)


def along(v, quad, step):
    shift = (-32 * step) % LANES
    here = pltpu.roll(v[quad], shift, 1)
    other = quad + (1 if step > 0 else -1)
    lanes = lanes_of(here.shape)
    own = lanes < LANES - 32 * step if step > 0 else lanes >= -32 * step
    if 0 <= other < len(v):
        return jnp.where(own, here, pltpu.roll(v[other], shift, 1))
    return jnp.where(own, here, 0.0)


def beside(v, quad, step):
    here = v[quad]
    rows, columns = rows_of(here.shape), lanes_of(here.shape) % 32
    total = along(v, quad, step) + along(v, quad, -step)
    total = total + jnp.where(rows < step, 0.0, pltpu.roll(here, step, 0))
    total = total + jnp.where(rows >= 32 - step, 0.0, pltpu.roll(here, 32 - step, 0))
    total = total + jnp.where(columns < step, 0.0, pltpu.roll(here, step, 1))
    return total + jnp.where(columns >= 32 - step, 0.0, pltpu.roll(here, LANES - step, 1))


def operated(v, quad):
    return screening * v[quad] - (beside(v, quad, 1) - 6.0 * v[quad])


def pair_sum(v, step, axis):
    index = (rows_of(v.shape), lanes_of(v.shape))[axis] // step
    other = v.shape[axis] - step
    return v + jnp.where(index % 2 == 0, pltpu.roll(v, other, axis), pltpu.roll(v, step, axis))


def square_sum(v):
    return pair_sum(pair_sum(v, 1, 1), 1, 0)


def cell_mean(v):
    return square_sum(pair_sum(v, 32, 1)) * 0.125


def in_plane(v):
    rows, columns = rows_of(v.shape), lanes_of(v.shape) % 32
    total = jnp.where(rows == 0, 0.0, pltpu.roll(v, 1, 0))
    total = total + jnp.where(rows == 31, 0.0, pltpu.roll(v, 31, 0))
    total = total + jnp.where(columns == 0, 0.0, pltpu.roll(v, 1, 1))
    return total + jnp.where(columns == 31, 0.0, pltpu.roll(v, LANES - 1, 1))


def source_of(even, uneven):
    low_half = lanes_of((16, LANES)) < 64
    top = jnp.where(low_half, even, pltpu.roll(uneven, 64, 1))
    bottom = jnp.where(low_half, pltpu.roll(even, 64, 1), uneven)
    return jnp.concatenate([top, bottom], axis=0)


def widen():
    square = (LANES, LANES)
    return jnp.where(rows_of(square) == lanes_of(square) // 4, 1.0, 0.0).astype(jnp.float32)


scale = damping / (screening + 6.0)
scale_b = damping / (screening + 1.5)
factor = time_step * long_range
edge_share = 0.125 * scale_b * (0.25 * scale_b) ** 2 * scale**2 * factor


def edge_kernel(own_ref, edge_ref, guess_s):
    groups, group = lax.axis_size("grp"), lax.axis_index("grp")
    quads, block = groups // 2, 32 // groups
    up = group == 0
    at = 16 + jnp.where(up, (quads - 1) * block, 0)
    for g in range(groups):
        guess_s[g * block : (g + 1) * block] = own_ref[g, pl.ds(pl.multiple_of(at, block), block)]
    guess = guess_s[...]
    source = jnp.where(
        up,
        source_of(own_ref[groups - 2, 0:16], own_ref[groups - 1, 0:16]),
        source_of(own_ref[0, 0:16], own_ref[1, 0:16]),
    )
    inner = jnp.where(up, pltpu.roll(guess, 32, 1), pltpu.roll(guess, LANES - 32, 1))
    flat = in_plane(guess)
    pre = guess + scale * (source - (screening * guess - (flat + inner - 6.0 * guess)))
    value = square_sum(pre + scale * (flat - (screening + 5.0) * guess))
    value = jnp.where(up, pltpu.roll(value, 32, 1), value)
    edge_ref[...] = edge_share * exact_dot(value, widen())


def edge_of(own):
    return pl.pallas_call(
        edge_kernel,
        out_shape=jax.ShapeDtypeStruct((32, LANES), jnp.float32),
        in_specs=[VMEM],
        out_specs=VMEM,
        scratch_shapes=[pltpu.VMEM((32, LANES), jnp.float32)],
        cost_estimate=pl.CostEstimate(flops=500_000, bytes_accessed=80_000, transcendentals=0),
        compiler_params=PARAMS,
        name="edge",
    )(own)


def solve_kernel(edged, own_ref, core_ref, chip_ref, wide_ref, rows_ref, guess_s, window_s):
    groups = lax.axis_size("grp")
    slab, slabs, group = lax.axis_index("slab"), lax.axis_size("slab"), lax.axis_index("grp")
    quads = groups // 2
    block = 32 // groups
    odd = lax.rem(slab, 2) == 1

    def low(*at):
        return jnp.where(odd, core_ref[at], chip_ref[at])

    def high(*at):
        return jnp.where(odd, chip_ref[at], core_ref[at])

    def own(*at):
        return own_ref[at]

    source = []

    def take(read, quad):
        at = len(source)
        source.append(source_of(read(2 * quad, pl.ds(0, 16)), read(2 * quad + 1, pl.ds(0, 16))))
        for g in range(groups):
            guess_s[at, g * block : (g + 1) * block] = read(g, pl.ds(16 + quad * block, block))

    near, trim = (quads, 0) if edged else (HALO, 1)
    for quad in range(quads - near, quads):
        take(low, quad)
    for quad in range(quads):
        take(own, quad)
    for quad in range(near):
        take(high, quad)
    total = quads + 2 * near
    has_low = jnp.where(slab > 0, 1.0, 0.0)
    has_high = jnp.where(slab < slabs - 1, 1.0, 0.0)

    def kept(v, quad):
        if quad < near:
            return v * has_low
        return v if quad < near + quads else v * has_high

    guess = [guess_s[quad] for quad in range(total)]
    pre = [
        kept(guess[quad] + scale * (source[quad] - operated(guess, quad)), quad)
        for quad in range(total)
    ]
    coarsest = [
        kept(cell_mean(source[quad] - operated(pre, quad)), quad)
        for quad in range(trim, total - trim)
    ]
    correction = [scale_b * v for v in coarsest]
    for sweep in range(NCOARSE - 1):
        last = sweep == NCOARSE - 2
        updated = []
        for quad in range(len(correction)):
            if last and quad in (0, len(correction) - 1):
                updated.append(None)
                continue
            c = correction[quad]
            applied = screening * c - 0.25 * (beside(correction, quad, 2) - 6.0 * c)
            updated.append(kept(c + scale_b * (coarsest[quad] - applied), quad + trim))
        correction = updated
    start = near - 1
    found = [pre[quad] + correction[quad - trim] for quad in range(start, total - start)]
    for _ in range(NPOST):
        found = [
            kept(v + scale * (source[quad + start] - operated(found, quad)), quad + start)
            for quad, v in enumerate(found)
        ]

    for quad in range(len(found)):
        window_s[quad] = found[quad]
    for quad in range(quads):
        rows_ref[quad] = window_s[quad + 1, pl.ds(pl.multiple_of(group * block, block), block), :]

    picked = []
    for i in range(4):
        at = 2 * group + 3 + i
        picked.append(
            pltpu.roll(window_s[at // QUAD], lax.rem(LANES - 32 * lax.rem(at, QUAD), LANES), 1)
        )
    if edged:
        lowest = group == 0
        facing = jnp.where(lowest, guess[0], pltpu.roll(guess[total - 1], 32, 1))
        reach = jnp.where(lowest, slab, slabs - 1 - slab) >= 2
        picked.append(jnp.where(reach, edge_share * scale / factor, 0.0) * square_sum(facing))
    wide = factor * exact_dot(jnp.concatenate(picked, axis=0), widen())
    wide = [wide[32 * i : 32 * (i + 1)] for i in range(len(picked))]
    if edged:
        wide[0] = wide[0] + jnp.where(group == 0, 1.0, 0.0) * wide[4]
        wide[3] = wide[3] + jnp.where(group == groups - 1, 1.0, 0.0) * wide[4]
    for i in range(4):
        wide_ref[i] = wide[i]


def solve(own, core, chip, guess, edged):
    groups = own.shape[0]
    quads = groups // 2
    total = 3 * quads if edged else quads + 2 * HALO
    return pl.pallas_call(
        functools.partial(solve_kernel, edged),
        out_shape=(
            jax.ShapeDtypeStruct((4, 32, LANES), jnp.float32),
            jax.ShapeDtypeStruct((quads, guess.shape[1], LANES), jnp.float32),
        ),
        in_specs=[VMEM] * 3,
        out_specs=(VMEM, VMEM),
        scratch_shapes=[
            pltpu.VMEM((total, 32, LANES), jnp.float32),
            pltpu.VMEM((quads + 2, 32, LANES), jnp.float32),
        ],
        cost_estimate=pl.CostEstimate(flops=6_000_000, bytes_accessed=500_000, transcendentals=0),
        compiler_params=PARAMS,
        name="solve",
    )(own, core, chip)


def finish_kernel(base_ref, wide_ref, rows_ref, *refs):
    edge_ref = refs[0] if len(refs) == 3 else None
    next_ref, potential_ref = refs[-2:]
    group, groups = lax.axis_index("grp"), lax.axis_size("grp")
    for quad in range(rows_ref.shape[0]):
        for i in range(QUAD):
            potential_ref[QUAD * quad + i] = rows_ref[quad, :, 32 * i : 32 * (i + 1)]
    wide = [wide_ref[i] for i in range(4)]
    if edge_ref is not None:
        wide[0] = wide[0] + jnp.where(group == 0, 1.0, 0.0) * edge_ref[...]
        wide[3] = wide[3] + jnp.where(group == groups - 1, 1.0, 0.0) * edge_ref[...]
    rows, lanes = rows_of((32, LANES)), lanes_of((32, LANES))
    for coarse in range(2):
        here = wide[coarse + 1]
        across = jnp.where(lanes == 0, 0.0, pltpu.roll(here, 1, 1))
        across = across + jnp.where(lanes == LANES - 1, 0.0, pltpu.roll(here, LANES - 1, 1))
        middle = across - 2.0 * here
        before = middle + (jnp.where(rows == 0, 0.0, pltpu.roll(here, 1, 0)) - here)
        after = middle + (jnp.where(rows == 31, 0.0, pltpu.roll(here, 31, 0)) - here)
        down = wide[coarse] - here
        up = wide[coarse + 2] - here
        for f in range(4):
            for j in range(4):
                term = (before, middle, middle, after)[j]
                if f == 0:
                    term = term + down
                if f == 3:
                    term = term + up
                at = (4 * coarse + f, pl.ds(j, 32, stride=4), slice(None))
                next_ref[at] = base_ref[at] + term


def finish(base, wide, rows, edge, guess):
    operands = [base, wide, rows] + ([] if edge is None else [edge])
    return pl.pallas_call(
        finish_kernel,
        out_shape=(
            jax.ShapeDtypeStruct(base.shape, jnp.float32),
            jax.ShapeDtypeStruct(guess.shape, jnp.float32),
        ),
        in_specs=[VMEM] * len(operands),
        out_specs=(VMEM, VMEM),
        cost_estimate=pl.CostEstimate(flops=500_000, bytes_accessed=1_100_000, transcendentals=0),
        compiler_params=PARAMS,
        name="finish",
    )(*operands)


def swaps(count, first=0):
    return [p for i in range(first, count - 1, 2) for p in ((i, i + 1), (i + 1, i))]


def per_device(comp, guess):
    slabs, groups = lax.axis_size("slab"), lax.axis_size("grp")
    group = lax.axis_index("grp")
    both = ("slab", "grp")
    devices = slabs * groups
    quads = groups // 2

    message, first, second = pack(comp, guess)

    bundle = jnp.zeros((groups,) + message.shape, jnp.float32)
    bundle = lax.dynamic_update_slice(bundle, message[None], (group, 0, 0))
    for k in range(1, groups):
        block = lax.ppermute(message, "grp", [(i, i ^ k) for i in range(groups)])
        bundle = lax.dynamic_update_slice(bundle, block[None], (group ^ k, 0, 0))

    first = lax.ppermute(first, both, swaps(devices))
    second = lax.ppermute(second, both, swaps(devices, 1))

    core = lax.ppermute(bundle, "slab", swaps(slabs))
    chip = lax.ppermute(bundle, "slab", swaps(slabs, 1))
    edge = None
    if quads < HALO:
        pairs = []
        for i in range(slabs - 2):
            pairs.append((i * groups, (i + 2) * groups))
            pairs.append(((i + 2) * groups + groups - 1, i * groups + groups - 1))
        edge = lax.ppermute(edge_of(bundle), both, pairs)

    base = base_of(comp, first, second)
    wide, rows = solve(bundle, core, chip, guess, edge is not None)
    return finish(base, wide, rows, edge, guess)


def solution(mesh):
    placed = (P(("slab", "grp"), None, None), P("slab", "grp", None))
    return jax.shard_map(per_device, mesh=mesh, in_specs=placed, out_specs=placed, check_vma=False)
```

```python
import functools

import jax
import jax.numpy as jnp
from jax import lax
from jax.experimental import pallas as pl
from jax.experimental.pallas import tpu as pltpu
from jax.sharding import PartitionSpec as P

NCOARSE = 3
NPOST = 2

gradient_energy = 0.5
screening = 0.5
damping = 0.8
long_range = 4.0
time_step = 0.02

LANES = 128
QUAD = 4
HALO = 3

VMEM = pl.BlockSpec(memory_space=pltpu.VMEM)
PARAMS = pltpu.CompilerParams(vmem_limit_bytes=8 * 2**20)


def lanes_of(shape):
    return lax.broadcasted_iota(jnp.int32, shape, len(shape) - 1)


def rows_of(shape):
    return lax.broadcasted_iota(jnp.int32, shape, len(shape) - 2)


def exact_dot(a, b):
    return jnp.dot(a, b, preferred_element_type=jnp.float32, precision=lax.Precision.HIGHEST)


def pack_guess_kernel(guess_ref, packed_ref):
    planes, rows, columns = guess_ref.shape
    for quad in range(planes // QUAD):
        at = quad * rows
        for i in range(QUAD):
            packed_ref[at : at + rows, i * columns : (i + 1) * columns] = guess_ref[QUAD * quad + i]


def pack_guess(guess):
    return pl.pallas_call(
        pack_guess_kernel,
        out_shape=jax.ShapeDtypeStruct((16, LANES), jnp.float32),
        in_specs=[VMEM],
        out_specs=VMEM,
        cost_estimate=pl.CostEstimate(flops=10_000, bytes_accessed=40_000, transcendentals=0),
        compiler_params=PARAMS,
        name="pack_guess",
    )(guess)


def pack_kernel(comp_ref, guess_ref, message_ref, first_ref, second_ref):
    columns = 32
    rows = comp_ref.shape[1] // 4
    half = rows // 2
    message_ref[half:, :] = guess_ref[...]
    pooled = []
    for plane in range(comp_ref.shape[0] // 4):
        total = None
        for i in range(4):
            for j in range(4):
                part = comp_ref[4 * plane + i, pl.ds(j, rows, stride=4), :]
                total = part if total is None else total + part
        pooled.append(total)
    stacked = jnp.concatenate(
        [pooled[0][:half], pooled[1][:half], pooled[0][half:], pooled[1][half:]], axis=0
    )
    square = (comp_ref.shape[2], LANES)
    pool = jnp.where(rows_of(square) // 4 == lanes_of(square) % columns, 1.0 / 64.0, 0.0)
    spread = exact_dot(stacked, pool.astype(jnp.float32))
    where = lanes_of((half, LANES)) // columns
    packed = spread[:half]
    for block in range(1, QUAD):
        packed = jnp.where(where == block, spread[block * half : (block + 1) * half], packed)
    message_ref[0:half, :] = packed
    odd = lax.rem(lax.axis_index("grp"), 2)
    top = comp_ref.shape[0] - 2
    first_ref[...] = comp_ref[pl.ds(top * (1 - odd), 2)]
    second_ref[...] = comp_ref[pl.ds(top * odd, 2)]


def pack(comp, guess):
    outer = jax.ShapeDtypeStruct((2,) + comp.shape[1:], jnp.float32)
    message = jax.ShapeDtypeStruct((32, LANES), jnp.float32)
    return pl.pallas_call(
        pack_kernel,
        out_shape=(message, outer, outer),
        in_specs=[VMEM] * 2,
        out_specs=(VMEM,) * 3,
        cost_estimate=pl.CostEstimate(flops=2_000_000, bytes_accessed=800_000, transcendentals=0),
        compiler_params=PARAMS,
        name="pack",
    )(comp, pack_guess(guess))


def beside_in_plane(v):
    rows, lanes = rows_of(v.shape), lanes_of(v.shape)
    last_row, last_lane = v.shape[0] - 1, v.shape[1] - 1
    total = jnp.where(rows == 0, 0.0, pltpu.roll(v, 1, 0))
    total = total + jnp.where(rows == last_row, 0.0, pltpu.roll(v, last_row, 0))
    total = total + jnp.where(lanes == 0, 0.0, pltpu.roll(v, 1, 1))
    return total + jnp.where(lanes == last_lane, 0.0, pltpu.roll(v, last_lane, 1))


def base_kernel(comp_ref, first_ref, second_ref, base_ref, chem_ref):
    planes = comp_ref.shape[0]
    group, groups = lax.axis_index("grp"), lax.axis_size("grp")
    index = lax.axis_index("slab") * groups + group
    devices = lax.axis_size("slab") * groups
    odd = lax.rem(group, 2) == 1

    below = jnp.where(index > 0, 1.0, 0.0)
    above = jnp.where(index < devices - 1, 1.0, 0.0)

    def plane(f):
        if f < 0:
            return jnp.where(odd, first_ref[f + 2], second_ref[f + 2]) * below
        if f >= planes:
            return jnp.where(odd, second_ref[f - planes], first_ref[f - planes]) * above
        return comp_ref[f]

    for f in range(-1, planes + 1):
        c = plane(f)
        beside = beside_in_plane(c) + plane(f - 1) + plane(f + 1)
        chem = c * c * c - c - gradient_energy * (beside - 6.0 * c)
        if f < 0:
            chem = chem * below
        if f >= planes:
            chem = chem * above
        chem_ref[f + 1] = chem
    for f in range(planes):
        v = chem_ref[f + 1]
        beside = beside_in_plane(v) + chem_ref[f] + chem_ref[f + 2]
        base_ref[f] = comp_ref[f] + time_step * (beside - 6.0 * v)


def base_of(comp, first, second):
    return pl.pallas_call(
        base_kernel,
        out_shape=jax.ShapeDtypeStruct(comp.shape, jnp.float32),
        in_specs=[VMEM] * 3,
        out_specs=VMEM,
        scratch_shapes=[pltpu.VMEM((comp.shape[0] + 2,) + comp.shape[1:], jnp.float32)],
        cost_estimate=pl.CostEstimate(flops=6_000_000, bytes_accessed=1_500_000, transcendentals=0),
        compiler_params=PARAMS,
        name="base",
    )(comp, first, second)


def along(v, quad, step):
    shift = (-32 * step) % LANES
    here = pltpu.roll(v[quad], shift, 1)
    other = quad + (1 if step > 0 else -1)
    lanes = lanes_of(here.shape)
    own = lanes < LANES - 32 * step if step > 0 else lanes >= -32 * step
    if 0 <= other < len(v):
        return jnp.where(own, here, pltpu.roll(v[other], shift, 1))
    return jnp.where(own, here, 0.0)


def beside(v, quad, step):
    here = v[quad]
    rows, columns = rows_of(here.shape), lanes_of(here.shape) % 32
    total = along(v, quad, step) + along(v, quad, -step)
    total = total + jnp.where(rows < step, 0.0, pltpu.roll(here, step, 0))
    total = total + jnp.where(rows >= 32 - step, 0.0, pltpu.roll(here, 32 - step, 0))
    total = total + jnp.where(columns < step, 0.0, pltpu.roll(here, step, 1))
    return total + jnp.where(columns >= 32 - step, 0.0, pltpu.roll(here, LANES - step, 1))


def operated(v, quad):
    return screening * v[quad] - (beside(v, quad, 1) - 6.0 * v[quad])


def pair_sum(v, step, axis):
    index = (rows_of(v.shape), lanes_of(v.shape))[axis] // step
    other = v.shape[axis] - step
    return v + jnp.where(index % 2 == 0, pltpu.roll(v, other, axis), pltpu.roll(v, step, axis))


def square_sum(v):
    return pair_sum(pair_sum(v, 1, 1), 1, 0)


def cell_mean(v):
    return square_sum(pair_sum(v, 32, 1)) * 0.125


def in_plane(v):
    rows, columns = rows_of(v.shape), lanes_of(v.shape) % 32
    total = jnp.where(rows == 0, 0.0, pltpu.roll(v, 1, 0))
    total = total + jnp.where(rows == 31, 0.0, pltpu.roll(v, 31, 0))
    total = total + jnp.where(columns == 0, 0.0, pltpu.roll(v, 1, 1))
    return total + jnp.where(columns == 31, 0.0, pltpu.roll(v, LANES - 1, 1))


def source_of(even, uneven):
    low_half = lanes_of((16, LANES)) < 64
    top = jnp.where(low_half, even, pltpu.roll(uneven, 64, 1))
    bottom = jnp.where(low_half, pltpu.roll(even, 64, 1), uneven)
    return jnp.concatenate([top, bottom], axis=0)


def widen():
    square = (LANES, LANES)
    return jnp.where(rows_of(square) == lanes_of(square) // 4, 1.0, 0.0).astype(jnp.float32)


scale = damping / (screening + 6.0)
scale_b = damping / (screening + 1.5)
factor = time_step * long_range
edge_share = 0.125 * scale_b * (0.25 * scale_b) ** 2 * scale**2 * factor


def edge_kernel(own_ref, edge_ref, guess_s):
    groups, group = lax.axis_size("grp"), lax.axis_index("grp")
    quads, block = groups // 2, 32 // groups
    up = group == groups - 1
    at = 16 + jnp.where(up, (quads - 1) * block, 0)
    for g in range(groups):
        guess_s[g * block : (g + 1) * block] = own_ref[g, pl.ds(pl.multiple_of(at, block), block)]
    guess = guess_s[...]
    source = jnp.where(
        up,
        source_of(own_ref[groups - 2, 0:16], own_ref[groups - 1, 0:16]),
        source_of(own_ref[0, 0:16], own_ref[1, 0:16]),
    )
    inner = jnp.where(up, pltpu.roll(guess, 32, 1), pltpu.roll(guess, LANES - 32, 1))
    flat = in_plane(guess)
    pre = guess + scale * (source - (screening * guess - (flat + inner - 6.0 * guess)))
    value = square_sum(pre + scale * (flat - (screening + 5.0) * guess))
    value = jnp.where(up, pltpu.roll(value, 32, 1), value)
    edge_ref[...] = edge_share * exact_dot(value, widen())


def edge_of(own):
    return pl.pallas_call(
        edge_kernel,
        out_shape=jax.ShapeDtypeStruct((32, LANES), jnp.float32),
        in_specs=[VMEM],
        out_specs=VMEM,
        scratch_shapes=[pltpu.VMEM((32, LANES), jnp.float32)],
        cost_estimate=pl.CostEstimate(flops=500_000, bytes_accessed=80_000, transcendentals=0),
        compiler_params=PARAMS,
        name="edge",
    )(own)


def solve_kernel(edged, own_ref, core_ref, chip_ref, wide_ref, rows_ref, guess_s, window_s):
    groups = lax.axis_size("grp")
    slab, slabs, group = lax.axis_index("slab"), lax.axis_size("slab"), lax.axis_index("grp")
    quads = groups // 2
    block = 32 // groups
    odd = lax.rem(slab, 2) == 1

    def low(*at):
        return jnp.where(odd, core_ref[at], chip_ref[at])

    def high(*at):
        return jnp.where(odd, chip_ref[at], core_ref[at])

    def own(*at):
        return own_ref[at]

    source = []

    def take(read, quad):
        at = len(source)
        source.append(source_of(read(2 * quad, pl.ds(0, 16)), read(2 * quad + 1, pl.ds(0, 16))))
        for g in range(groups):
            guess_s[at, g * block : (g + 1) * block] = read(g, pl.ds(16 + quad * block, block))

    near, trim = (quads, 0) if edged else (HALO, 1)
    for quad in range(quads - near, quads):
        take(low, quad)
    for quad in range(quads):
        take(own, quad)
    for quad in range(near):
        take(high, quad)
    total = quads + 2 * near
    has_low = jnp.where(slab > 0, 1.0, 0.0)
    has_high = jnp.where(slab < slabs - 1, 1.0, 0.0)

    def kept(v, quad):
        if quad < near:
            return v * has_low
        return v if quad < near + quads else v * has_high

    guess = [kept(guess_s[quad], quad) for quad in range(total)]
    pre = [
        kept(guess[quad] + scale * (source[quad] - operated(guess, quad)), quad)
        for quad in range(total)
    ]
    coarsest = [
        kept(cell_mean(source[quad] - operated(pre, quad)), quad)
        for quad in range(trim, total - trim)
    ]
    correction = [scale_b * v for v in coarsest]
    for sweep in range(NCOARSE - 1):
        last = sweep == NCOARSE - 2
        updated = []
        for quad in range(len(correction)):
            if last and quad in (0, len(correction) - 1):
                updated.append(None)
                continue
            c = correction[quad]
            applied = screening * c - 0.25 * (beside(correction, quad, 2) - 6.0 * c)
            updated.append(kept(c + scale_b * (coarsest[quad] - applied), quad + trim))
        correction = updated
    start = near - 1
    found = [pre[quad] + correction[quad - trim] for quad in range(start, total - start)]
    for _ in range(NPOST):
        found = [
            kept(v + scale * (source[quad + start] - operated(found, quad)), quad + start)
            for quad, v in enumerate(found)
        ]

    for quad in range(len(found)):
        window_s[quad] = found[quad]
    for quad in range(quads):
        rows_ref[quad] = window_s[quad + 1, pl.ds(pl.multiple_of(group * block, block), block), :]

    picked = []
    for i in range(4):
        at = 2 * group + 3 + i
        picked.append(
            pltpu.roll(window_s[at // QUAD], lax.rem(LANES - 32 * lax.rem(at, QUAD), LANES), 1)
        )
    if edged:
        lowest = group == 0
        facing = jnp.where(lowest, guess[0], pltpu.roll(guess[total - 1], 32, 1))
        reach = jnp.where(lowest, slab, slabs - 1 - slab) >= 2
        picked.append(jnp.where(reach, edge_share * scale / factor, 0.0) * square_sum(facing))
    wide = factor * exact_dot(jnp.concatenate(picked, axis=0), widen())
    wide = [wide[32 * i : 32 * (i + 1)] for i in range(len(picked))]
    if edged:
        wide[0] = wide[0] + jnp.where(group == 0, 1.0, 0.0) * wide[4]
        wide[3] = wide[3] + jnp.where(group == groups - 1, 1.0, 0.0) * wide[4]
    for i in range(4):
        wide_ref[i] = wide[i]


def solve(own, core, chip, guess, edged):
    groups = own.shape[0]
    quads = groups // 2
    total = 3 * quads if edged else quads + 2 * HALO
    return pl.pallas_call(
        functools.partial(solve_kernel, edged),
        out_shape=(
            jax.ShapeDtypeStruct((4, 32, LANES), jnp.float32),
            jax.ShapeDtypeStruct((quads, guess.shape[1], LANES), jnp.float32),
        ),
        in_specs=[VMEM] * 3,
        out_specs=(VMEM, VMEM),
        scratch_shapes=[
            pltpu.VMEM((total, 32, LANES), jnp.float32),
            pltpu.VMEM((quads + 2, 32, LANES), jnp.float32),
        ],
        cost_estimate=pl.CostEstimate(flops=6_000_000, bytes_accessed=500_000, transcendentals=0),
        compiler_params=PARAMS,
        name="solve",
    )(own, core, chip)


def finish_kernel(base_ref, wide_ref, rows_ref, *refs):
    edge_ref = refs[0] if len(refs) == 3 else None
    next_ref, potential_ref = refs[-2:]
    group, groups = lax.axis_index("grp"), lax.axis_size("grp")
    slab, slabs = lax.axis_index("slab"), lax.axis_size("slab")
    for quad in range(rows_ref.shape[0]):
        for i in range(QUAD):
            potential_ref[QUAD * quad + i] = rows_ref[quad, :, 32 * i : 32 * (i + 1)]
    wide = [wide_ref[i] for i in range(4)]
    if edge_ref is not None:
        lowest = (group == 0) & (slab >= 2)
        highest = (group == groups - 1) & (slab < slabs - 2)
        wide[0] = wide[0] + jnp.where(lowest, 1.0, 0.0) * edge_ref[...]
        wide[3] = wide[3] + jnp.where(highest, 1.0, 0.0) * edge_ref[...]
    rows, lanes = rows_of((32, LANES)), lanes_of((32, LANES))
    for coarse in range(2):
        here = wide[coarse + 1]
        across = jnp.where(lanes == 0, 0.0, pltpu.roll(here, 1, 1))
        across = across + jnp.where(lanes == LANES - 1, 0.0, pltpu.roll(here, LANES - 1, 1))
        middle = across - 2.0 * here
        before = middle + (jnp.where(rows == 0, 0.0, pltpu.roll(here, 1, 0)) - here)
        after = middle + (jnp.where(rows == 31, 0.0, pltpu.roll(here, 31, 0)) - here)
        down = wide[coarse] - here
        up = wide[coarse + 2] - here
        for f in range(4):
            for j in range(4):
                term = (before, middle, middle, after)[j]
                if f == 0:
                    term = term + down
                if f == 3:
                    term = term + up
                at = (4 * coarse + f, pl.ds(j, 32, stride=4), slice(None))
                next_ref[at] = base_ref[at] + term


def finish(base, wide, rows, edge, guess):
    operands = [base, wide, rows] + ([] if edge is None else [edge])
    return pl.pallas_call(
        finish_kernel,
        out_shape=(
            jax.ShapeDtypeStruct(base.shape, jnp.float32),
            jax.ShapeDtypeStruct(guess.shape, jnp.float32),
        ),
        in_specs=[VMEM] * len(operands),
        out_specs=(VMEM, VMEM),
        cost_estimate=pl.CostEstimate(flops=500_000, bytes_accessed=1_100_000, transcendentals=0),
        compiler_params=PARAMS,
        name="finish",
    )(*operands)


def pairing(*pairs):
    return [p for a, b in pairs for p in {(a, b), (b, a)}]


def per_device(comp, guess):
    slabs, groups = lax.axis_size("slab"), lax.axis_size("grp")
    group = lax.axis_index("grp")
    both = ("slab", "grp")
    devices = slabs * groups
    quads = groups // 2

    def at(slab, member):
        return slab * groups + member

    message, first, second = pack(comp, guess)


    bundle = jnp.zeros((groups,) + message.shape, jnp.float32)
    bundle = lax.dynamic_update_slice(bundle, message[None], (group, 0, 0))
    for k in range(1, groups):
        block = lax.ppermute(message, "grp", [(i, i ^ k) for i in range(groups)])
        bundle = lax.dynamic_update_slice(bundle, block[None], (group ^ k, 0, 0))

    first = lax.ppermute(first, both, pairing(*((d, d + 1) for d in range(0, devices, 2))))
    second = lax.ppermute(
        second,
        both,
        pairing(
            *((d, d + 1) for d in range(1, devices - 1, 2)), *idle_second(devices)
        ),
    )

    core = lax.ppermute(bundle, "slab", pairing(*((i, i + 1) for i in range(0, slabs, 2))))
    chip = lax.ppermute(
        bundle,
        both,
        pairing(
            *((at(i, g), at(i + 1, g)) for i in range(1, slabs - 1, 2) for g in range(groups)),
            *idle_chip(at, slabs, groups),
        ),
    )
    edge = None
    if quads < HALO:
        edge = lax.ppermute(edge_of(bundle), both, edge_pairs(at, slabs, groups))

    base = base_of(comp, first, second)
    wide, rows = solve(bundle, core, chip, guess, edge is not None)
    return finish(base, wide, rows, edge, guess)


def idle_second(devices):
    return [(0, 0), (devices - 1, devices - 1)]


def idle_chip(at, slabs, groups):
    half = groups // 2
    return [(at(s, g), at(s, g + half)) for s in (0, slabs - 1) for g in range(half)]


def edge_pairs(at, slabs, groups):
    top = groups - 1
    return pairing(
        *((at(i, top), at(i + 2, 0)) for i in range(slabs - 2)),
        *((at(i, g), at(i + 1, g)) for i in range(0, slabs, 2) for g in range(1, top)),
        (at(0, 0), at(1, 0)),
        (at(slabs - 2, top), at(slabs - 1, top)),
    )


def solution(mesh):
    placed = (P(("slab", "grp"), None, None), P("slab", "grp", None))
    return jax.shard_map(per_device, mesh=mesh, in_specs=placed, out_specs=placed, check_vma=False)
```

```python
import functools

import jax
import jax.numpy as jnp
from jax import lax
from jax.experimental import pallas as pl
from jax.experimental.pallas import tpu as pltpu
from jax.sharding import PartitionSpec as P

NCOARSE = 3
NPOST = 2

gradient_energy = 0.5
screening = 0.5
damping = 0.8
long_range = 4.0
time_step = 0.02

LANES = 128
QUAD = 4
HALO = 3

POOL_FLOPS = 300_000_000

VMEM = pl.BlockSpec(memory_space=pltpu.VMEM)
PARAMS = pltpu.CompilerParams(vmem_limit_bytes=8 * 2**20)


def lanes_of(shape):
    return lax.broadcasted_iota(jnp.int32, shape, len(shape) - 1)


def rows_of(shape):
    return lax.broadcasted_iota(jnp.int32, shape, len(shape) - 2)


def exact_dot(a, b):
    return jnp.dot(a, b, preferred_element_type=jnp.float32, precision=lax.Precision.HIGHEST)


def pool_kernel(comp_ref, source_ref, first_ref, second_ref):
    columns = 32
    rows = comp_ref.shape[1] // 4
    half = rows // 2
    pooled = []
    for plane in range(comp_ref.shape[0] // 4):
        total = None
        for i in range(4):
            for j in range(4):
                part = comp_ref[4 * plane + i, pl.ds(j, rows, stride=4), :]
                total = part if total is None else total + part
        pooled.append(total)
    stacked = jnp.concatenate(
        [pooled[0][:half], pooled[1][:half], pooled[0][half:], pooled[1][half:]], axis=0
    )
    square = (comp_ref.shape[2], LANES)
    pool = jnp.where(rows_of(square) // 4 == lanes_of(square) % columns, 1.0 / 64.0, 0.0)
    spread = exact_dot(stacked, pool.astype(jnp.float32))
    where = lanes_of((half, LANES)) // columns
    packed = spread[:half]
    for block in range(1, QUAD):
        packed = jnp.where(where == block, spread[block * half : (block + 1) * half], packed)
    source_ref[...] = packed
    odd = lax.rem(lax.axis_index("grp"), 2)
    top = comp_ref.shape[0] - 2
    first_ref[...] = comp_ref[pl.ds(top * (1 - odd), 2)]
    second_ref[...] = comp_ref[pl.ds(top * odd, 2)]


def pack_kernel(source_ref, guess_ref, message_ref):
    message_ref[0:16, :] = source_ref[...]
    planes, rows, columns = guess_ref.shape
    for quad in range(planes // QUAD):
        at = 16 + quad * rows
        for i in range(QUAD):
            message_ref[at : at + rows, i * columns : (i + 1) * columns] = guess_ref[QUAD * quad + i]


def pack(comp, guess):
    outer = jax.ShapeDtypeStruct((2,) + comp.shape[1:], jnp.float32)
    source, first, second = pl.pallas_call(
        pool_kernel,
        out_shape=(jax.ShapeDtypeStruct((16, LANES), jnp.float32), outer, outer),
        in_specs=[VMEM],
        out_specs=(VMEM,) * 3,
        cost_estimate=pl.CostEstimate(
            flops=POOL_FLOPS, bytes_accessed=800_000, transcendentals=0
        ),
        compiler_params=PARAMS,
        name="pool",
    )(comp)
    message = pl.pallas_call(
        pack_kernel,
        out_shape=jax.ShapeDtypeStruct((32, LANES), jnp.float32),
        in_specs=[VMEM] * 2,
        out_specs=VMEM,
        cost_estimate=pl.CostEstimate(flops=10_000, bytes_accessed=40_000, transcendentals=0),
        compiler_params=PARAMS,
        name="pack",
    )(source, guess)
    return message, first, second


def beside_in_plane(v):
    rows, lanes = rows_of(v.shape), lanes_of(v.shape)
    last_row, last_lane = v.shape[0] - 1, v.shape[1] - 1
    total = jnp.where(rows == 0, 0.0, pltpu.roll(v, 1, 0))
    total = total + jnp.where(rows == last_row, 0.0, pltpu.roll(v, last_row, 0))
    total = total + jnp.where(lanes == 0, 0.0, pltpu.roll(v, 1, 1))
    return total + jnp.where(lanes == last_lane, 0.0, pltpu.roll(v, last_lane, 1))


def chem_of(below, c, above):
    beside = beside_in_plane(c) + below + above
    return c * c * c - c - gradient_energy * (beside - 6.0 * c)


def stepped(c, below, v, above):
    beside = beside_in_plane(v) + below + above
    return c + time_step * (beside - 6.0 * v)


def inner_kernel(comp_ref, base_ref, chem_ref):
    planes = comp_ref.shape[0]
    for f in range(1, planes - 1):
        chem_ref[f] = chem_of(comp_ref[f - 1], comp_ref[f], comp_ref[f + 1])
    for f in range(2, planes - 2):
        base_ref[f] = stepped(comp_ref[f], chem_ref[f - 1], chem_ref[f], chem_ref[f + 1])


def inner_of(comp):
    shape = jax.ShapeDtypeStruct(comp.shape, jnp.float32)
    return pl.pallas_call(
        inner_kernel,
        out_shape=(shape, shape),
        in_specs=[VMEM],
        out_specs=(VMEM, VMEM),
        cost_estimate=pl.CostEstimate(flops=3_000_000, bytes_accessed=1_500_000, transcendentals=0),
        compiler_params=PARAMS,
        name="inner",
    )(comp)


def outer_kernel(comp_ref, first_ref, second_ref, chem_ref, base_ref):
    planes = comp_ref.shape[0]
    group, groups = lax.axis_index("grp"), lax.axis_size("grp")
    index = lax.axis_index("slab") * groups + group
    devices = lax.axis_size("slab") * groups
    odd = lax.rem(group, 2) == 1
    below = jnp.where(index > 0, 1.0, 0.0)
    above = jnp.where(index < devices - 1, 1.0, 0.0)
    sides = (
        (0, 1, 2, below, first_ref, second_ref, 1, 0),
        (planes - 1, planes - 2, planes - 3, above, second_ref, first_ref, 0, 1),
    )
    for side, (edge, next_in, third, there, if_odd, if_even, near, far) in enumerate(sides):
        c, inner = comp_ref[edge], comp_ref[next_in]
        beyond = jnp.where(odd, if_odd[near], if_even[near]) * there
        further = jnp.where(odd, if_odd[far], if_even[far]) * there
        chem_beyond = chem_of(further, beyond, c) * there
        chem_edge = chem_of(beyond, c, inner)
        base_ref[3 * side] = stepped(c, chem_beyond, chem_edge, chem_ref[next_in])
        base_ref[1 + side] = stepped(inner, chem_edge, chem_ref[next_in], chem_ref[third])


def outer_of(comp, first, second, chem):
    return pl.pallas_call(
        outer_kernel,
        out_shape=jax.ShapeDtypeStruct((4,) + comp.shape[1:], jnp.float32),
        in_specs=[VMEM] * 4,
        out_specs=VMEM,
        cost_estimate=pl.CostEstimate(flops=3_000_000, bytes_accessed=1_500_000, transcendentals=0),
        compiler_params=PARAMS,
        name="outer",
    )(comp, first, second, chem)


def rolled(v, step):
    on = [pltpu.roll(here, LANES - 32 * step, 1) for here in v]
    back = on if 64 * step == LANES else [pltpu.roll(here, 32 * step, 1) for here in v]
    return on, back


def beside(v, quad, step, turned):
    here = v[quad]
    on, back = turned
    rows, lanes = rows_of(here.shape), lanes_of(here.shape)
    columns = lanes % 32
    next_quad = on[quad + 1] if quad + 1 < len(v) else 0.0
    last_quad = back[quad - 1] if quad else 0.0
    total = jnp.where(lanes < LANES - 32 * step, on[quad], next_quad)
    total = total + jnp.where(lanes >= 32 * step, back[quad], last_quad)
    total = total + jnp.where(rows < step, 0.0, pltpu.roll(here, step, 0))
    total = total + jnp.where(rows >= 32 - step, 0.0, pltpu.roll(here, 32 - step, 0))
    total = total + jnp.where(columns < step, 0.0, pltpu.roll(here, step, 1))
    return total + jnp.where(columns >= 32 - step, 0.0, pltpu.roll(here, LANES - step, 1))


def operated(v):
    turned = rolled(v, 1)
    return [
        screening * here - (beside(v, quad, 1, turned) - 6.0 * here) for quad, here in enumerate(v)
    ]


def pair_sum(v, step, axis):
    index = (rows_of(v.shape), lanes_of(v.shape))[axis] // step
    other = v.shape[axis] - step
    return v + jnp.where(index % 2 == 0, pltpu.roll(v, other, axis), pltpu.roll(v, step, axis))


def square_sum(v):
    return pair_sum(pair_sum(v, 1, 1), 1, 0)


def cell_mean(v):
    return square_sum(pair_sum(v, 32, 1)) * 0.125


def in_plane(v):
    rows, columns = rows_of(v.shape), lanes_of(v.shape) % 32
    total = jnp.where(rows == 0, 0.0, pltpu.roll(v, 1, 0))
    total = total + jnp.where(rows == 31, 0.0, pltpu.roll(v, 31, 0))
    total = total + jnp.where(columns == 0, 0.0, pltpu.roll(v, 1, 1))
    return total + jnp.where(columns == 31, 0.0, pltpu.roll(v, LANES - 1, 1))


def source_of(even, uneven):
    low_half = lanes_of((16, LANES)) < 64
    top = jnp.where(low_half, even, pltpu.roll(uneven, 64, 1))
    bottom = jnp.where(low_half, pltpu.roll(even, 64, 1), uneven)
    return jnp.concatenate([top, bottom], axis=0)


def widen():
    square = (LANES, LANES)
    return jnp.where(rows_of(square) == lanes_of(square) // 4, 1.0, 0.0).astype(jnp.float32)


scale = damping / (screening + 6.0)
scale_b = damping / (screening + 1.5)
factor = time_step * long_range
edge_share = 0.125 * scale_b * (0.25 * scale_b) ** 2 * scale**2 * factor


def edge_kernel(own_ref, edge_ref, guess_s):
    groups, group = lax.axis_size("grp"), lax.axis_index("grp")
    quads, block = groups // 2, 32 // groups
    up = group == groups - 1
    at = 16 + jnp.where(up, (quads - 1) * block, 0)
    for g in range(groups):
        guess_s[g * block : (g + 1) * block] = own_ref[g, pl.ds(pl.multiple_of(at, block), block)]
    guess = guess_s[...]
    source = jnp.where(
        up,
        source_of(own_ref[groups - 2, 0:16], own_ref[groups - 1, 0:16]),
        source_of(own_ref[0, 0:16], own_ref[1, 0:16]),
    )
    inner = jnp.where(up, pltpu.roll(guess, 32, 1), pltpu.roll(guess, LANES - 32, 1))
    flat = in_plane(guess)
    pre = guess + scale * (source - (screening * guess - (flat + inner - 6.0 * guess)))
    value = square_sum(pre + scale * (flat - (screening + 5.0) * guess))
    value = jnp.where(up, pltpu.roll(value, 32, 1), value)
    edge_ref[...] = edge_share * exact_dot(value, widen())


def edge_of(own):
    return pl.pallas_call(
        edge_kernel,
        out_shape=jax.ShapeDtypeStruct((32, LANES), jnp.float32),
        in_specs=[VMEM],
        out_specs=VMEM,
        scratch_shapes=[pltpu.VMEM((32, LANES), jnp.float32)],
        cost_estimate=pl.CostEstimate(flops=500_000, bytes_accessed=80_000, transcendentals=0),
        compiler_params=PARAMS,
        name="edge",
    )(own)


def solve_kernel(edged, own_ref, core_ref, chip_ref, wide_ref, rows_ref, guess_s, window_s):
    groups = lax.axis_size("grp")
    slab, slabs, group = lax.axis_index("slab"), lax.axis_size("slab"), lax.axis_index("grp")
    quads = groups // 2
    block = 32 // groups
    odd = lax.rem(slab, 2) == 1

    def low(*at):
        return jnp.where(odd, core_ref[at], chip_ref[at])

    def high(*at):
        return jnp.where(odd, chip_ref[at], core_ref[at])

    def own(*at):
        return own_ref[at]

    source = []

    def take(read, quad):
        at = len(source)
        source.append(source_of(read(2 * quad, pl.ds(0, 16)), read(2 * quad + 1, pl.ds(0, 16))))
        for g in range(groups):
            guess_s[at, g * block : (g + 1) * block] = read(g, pl.ds(16 + quad * block, block))

    near, trim = (quads, 0) if edged else (HALO, 1)
    for quad in range(quads - near, quads):
        take(low, quad)
    for quad in range(quads):
        take(own, quad)
    for quad in range(near):
        take(high, quad)
    total = quads + 2 * near
    has_low = jnp.where(slab > 0, 1.0, 0.0)
    has_high = jnp.where(slab < slabs - 1, 1.0, 0.0)

    def kept(v, quad):
        if quad < near:
            return v * has_low
        return v if quad < near + quads else v * has_high

    guess = [kept(guess_s[quad], quad) for quad in range(total)]
    applied = operated(guess)
    pre = [
        kept(guess[quad] + scale * (source[quad] - applied[quad]), quad) for quad in range(total)
    ]
    applied = operated(pre)
    coarsest = [
        kept(cell_mean(source[quad] - applied[quad]), quad) for quad in range(trim, total - trim)
    ]
    correction = [scale_b * v for v in coarsest]
    for sweep in range(NCOARSE - 1):
        last = sweep == NCOARSE - 2
        updated = []
        turned = rolled(correction, 2)
        for quad in range(len(correction)):
            if last and quad in (0, len(correction) - 1):
                updated.append(None)
                continue
            c = correction[quad]
            applied = screening * c - 0.25 * (beside(correction, quad, 2, turned) - 6.0 * c)
            updated.append(kept(c + scale_b * (coarsest[quad] - applied), quad + trim))
        correction = updated
    start = near - 1
    found = [pre[quad] + correction[quad - trim] for quad in range(start, total - start)]
    for _ in range(NPOST):
        applied = operated(found)
        found = [
            kept(v + scale * (source[quad + start] - applied[quad]), quad + start)
            for quad, v in enumerate(found)
        ]

    for quad in range(len(found)):
        window_s[quad] = found[quad]
    for quad in range(quads):
        rows_ref[quad] = window_s[quad + 1, pl.ds(pl.multiple_of(group * block, block), block), :]

    picked = []
    for i in range(4):
        at = 2 * group + 3 + i
        picked.append(
            pltpu.roll(window_s[at // QUAD], lax.rem(LANES - 32 * lax.rem(at, QUAD), LANES), 1)
        )
    if edged:
        lowest = group == 0
        facing = jnp.where(lowest, guess[0], pltpu.roll(guess[total - 1], 32, 1))
        reach = jnp.where(lowest, slab, slabs - 1 - slab) >= 2
        picked.append(jnp.where(reach, edge_share * scale / factor, 0.0) * square_sum(facing))
    wide = factor * exact_dot(jnp.concatenate(picked, axis=0), widen())
    wide = [wide[32 * i : 32 * (i + 1)] for i in range(len(picked))]
    if edged:
        wide[0] = wide[0] + jnp.where(group == 0, 1.0, 0.0) * wide[4]
        wide[3] = wide[3] + jnp.where(group == groups - 1, 1.0, 0.0) * wide[4]
    for i in range(4):
        wide_ref[i] = wide[i]


def solve(own, core, chip, guess, edged):
    groups = own.shape[0]
    quads = groups // 2
    total = 3 * quads if edged else quads + 2 * HALO
    return pl.pallas_call(
        functools.partial(solve_kernel, edged),
        out_shape=(
            jax.ShapeDtypeStruct((4, 32, LANES), jnp.float32),
            jax.ShapeDtypeStruct((quads, guess.shape[1], LANES), jnp.float32),
        ),
        in_specs=[VMEM] * 3,
        out_specs=(VMEM, VMEM),
        scratch_shapes=[
            pltpu.VMEM((total, 32, LANES), jnp.float32),
            pltpu.VMEM((quads + 2, 32, LANES), jnp.float32),
        ],
        cost_estimate=pl.CostEstimate(flops=6_000_000, bytes_accessed=500_000, transcendentals=0),
        compiler_params=PARAMS,
        name="solve",
    )(own, core, chip)


def finish_kernel(inner_ref, outer_ref, wide_ref, rows_ref, *refs):
    edge_ref = refs[0] if len(refs) == 3 else None
    next_ref, potential_ref = refs[-2:]
    group, groups = lax.axis_index("grp"), lax.axis_size("grp")
    slab, slabs = lax.axis_index("slab"), lax.axis_size("slab")
    for quad in range(rows_ref.shape[0]):
        for i in range(QUAD):
            potential_ref[QUAD * quad + i] = rows_ref[quad, :, 32 * i : 32 * (i + 1)]
    wide = [wide_ref[i] for i in range(4)]
    if edge_ref is not None:
        lowest = (group == 0) & (slab >= 2)
        highest = (group == groups - 1) & (slab < slabs - 2)
        wide[0] = wide[0] + jnp.where(lowest, 1.0, 0.0) * edge_ref[...]
        wide[3] = wide[3] + jnp.where(highest, 1.0, 0.0) * edge_ref[...]
    rows, lanes = rows_of((32, LANES)), lanes_of((32, LANES))
    for coarse in range(2):
        here = wide[coarse + 1]
        across = jnp.where(lanes == 0, 0.0, pltpu.roll(here, 1, 1))
        across = across + jnp.where(lanes == LANES - 1, 0.0, pltpu.roll(here, LANES - 1, 1))
        middle = across - 2.0 * here
        before = middle + (jnp.where(rows == 0, 0.0, pltpu.roll(here, 1, 0)) - here)
        after = middle + (jnp.where(rows == 31, 0.0, pltpu.roll(here, 31, 0)) - here)
        down = wide[coarse] - here
        up = wide[coarse + 2] - here
        for f in range(4):
            for j in range(4):
                term = (before, middle, middle, after)[j]
                if f == 0:
                    term = term + down
                if f == 3:
                    term = term + up
                plane, within = 4 * coarse + f, (pl.ds(j, 32, stride=4), slice(None))
                if 2 <= plane < 6:
                    base = inner_ref[(plane, *within)]
                else:
                    base = outer_ref[(plane % 4, *within)]
                next_ref[(plane, *within)] = base + term


def finish(inner, outer, wide, rows, edge, guess):
    operands = [inner, outer, wide, rows] + ([] if edge is None else [edge])
    return pl.pallas_call(
        finish_kernel,
        out_shape=(
            jax.ShapeDtypeStruct(inner.shape, jnp.float32),
            jax.ShapeDtypeStruct(guess.shape, jnp.float32),
        ),
        in_specs=[VMEM] * len(operands),
        out_specs=(VMEM, VMEM),
        cost_estimate=pl.CostEstimate(flops=500_000, bytes_accessed=1_100_000, transcendentals=0),
        compiler_params=PARAMS,
        name="finish",
    )(*operands)


def pairing(*pairs):
    return [p for a, b in pairs for p in {(a, b), (b, a)}]


def per_device(comp, guess):
    slabs, groups = lax.axis_size("slab"), lax.axis_size("grp")
    group = lax.axis_index("grp")
    both = ("slab", "grp")
    devices = slabs * groups
    quads = groups // 2

    def at(slab, member):
        return slab * groups + member

    message, first, second = pack(comp, guess)


    bundle = jnp.zeros((groups,) + message.shape, jnp.float32)
    bundle = lax.dynamic_update_slice(bundle, message[None], (group, 0, 0))
    for k in range(1, groups):
        block = lax.ppermute(message, "grp", [(i, i ^ k) for i in range(groups)])
        bundle = lax.dynamic_update_slice(bundle, block[None], (group ^ k, 0, 0))

    first = lax.ppermute(first, both, pairing(*((d, d + 1) for d in range(0, devices, 2))))
    second = lax.ppermute(
        second,
        both,
        pairing(
            *((d, d + 1) for d in range(1, devices - 1, 2)), *idle_second(devices)
        ),
    )

    core = lax.ppermute(bundle, "slab", pairing(*((i, i + 1) for i in range(0, slabs, 2))))
    chip = lax.ppermute(
        bundle,
        both,
        pairing(
            *((at(i, g), at(i + 1, g)) for i in range(1, slabs - 1, 2) for g in range(groups)),
            *idle_chip(at, slabs, groups),
        ),
    )
    edge = None
    if quads < HALO:
        edge = lax.ppermute(edge_of(bundle), both, edge_pairs(at, slabs, groups))

    inner, chem = inner_of(comp)
    wide, rows = solve(bundle, core, chip, guess, edge is not None)
    outer = outer_of(comp, first, second, chem)
    return finish(inner, outer, wide, rows, edge, guess)


def idle_second(devices):
    return [(0, 0), (devices - 1, devices - 1)]


def idle_chip(at, slabs, groups):
    half = groups // 2
    return [(at(s, g), at(s, g + half)) for s in (0, slabs - 1) for g in range(half)]


def edge_pairs(at, slabs, groups):
    top = groups - 1
    return pairing(
        *((at(i, top), at(i + 2, 0)) for i in range(slabs - 2)),
        *((at(i, g), at(i + 1, g)) for i in range(0, slabs, 2) for g in range(1, top)),
        (at(0, 0), at(1, 0)),
        (at(slabs - 2, top), at(slabs - 1, top)),
    )


def solution(mesh):
    placed = (P(("slab", "grp"), None, None), P("slab", "grp", None))
    return jax.shard_map(per_device, mesh=mesh, in_specs=placed, out_specs=placed, check_vma=False)
```

```python
import functools

import jax
import jax.numpy as jnp
from jax import lax
from jax.experimental import pallas as pl
from jax.experimental.pallas import tpu as pltpu
from jax.sharding import PartitionSpec as P

NCOARSE = 3
NPOST = 2

gradient_energy = 0.5
screening = 0.5
damping = 0.8
long_range = 4.0
time_step = 0.02

LANES = 128
QUAD = 4
HALO = 3

POOL_FLOPS = 300_000_000

VMEM = pl.BlockSpec(memory_space=pltpu.VMEM)
PARAMS = pltpu.CompilerParams(vmem_limit_bytes=8 * 2**20)


def lanes_of(shape):
    return lax.broadcasted_iota(jnp.int32, shape, len(shape) - 1)


def rows_of(shape):
    return lax.broadcasted_iota(jnp.int32, shape, len(shape) - 2)


def exact_dot(a, b):
    return jnp.dot(a, b, preferred_element_type=jnp.float32, precision=lax.Precision.HIGHEST)


def pool_kernel(comp_ref, source_ref, first_ref, second_ref):
    columns = 32
    rows = comp_ref.shape[1] // 4
    half = rows // 2
    pooled = []
    for plane in range(comp_ref.shape[0] // 4):
        total = None
        for i in range(4):
            for j in range(4):
                part = comp_ref[4 * plane + i, pl.ds(j, rows, stride=4), :]
                total = part if total is None else total + part
        pooled.append(total)
    stacked = jnp.concatenate(
        [pooled[0][:half], pooled[1][:half], pooled[0][half:], pooled[1][half:]], axis=0
    )
    square = (comp_ref.shape[2], LANES)
    pool = jnp.where(rows_of(square) // 4 == lanes_of(square) % columns, 1.0 / 64.0, 0.0)
    spread = exact_dot(stacked, pool.astype(jnp.float32))
    where = lanes_of((half, LANES)) // columns
    packed = spread[:half]
    for block in range(1, QUAD):
        packed = jnp.where(where == block, spread[block * half : (block + 1) * half], packed)
    source_ref[...] = packed
    odd = lax.rem(lax.axis_index("grp"), 2)
    top = comp_ref.shape[0] - 2
    first_ref[...] = comp_ref[pl.ds(top * (1 - odd), 2)]
    second_ref[...] = comp_ref[pl.ds(top * odd, 2)]


def pack_kernel(source_ref, guess_ref, message_ref):
    message_ref[0:16, :] = source_ref[...]
    planes, rows, columns = guess_ref.shape
    for quad in range(planes // QUAD):
        at = 16 + quad * rows
        for i in range(QUAD):
            message_ref[at : at + rows, i * columns : (i + 1) * columns] = guess_ref[QUAD * quad + i]


def pack(comp, guess):
    outer = jax.ShapeDtypeStruct((2,) + comp.shape[1:], jnp.float32)
    source, first, second = pl.pallas_call(
        pool_kernel,
        out_shape=(jax.ShapeDtypeStruct((16, LANES), jnp.float32), outer, outer),
        in_specs=[VMEM],
        out_specs=(VMEM,) * 3,
        cost_estimate=pl.CostEstimate(
            flops=POOL_FLOPS, bytes_accessed=800_000, transcendentals=0
        ),
        compiler_params=PARAMS,
        name="pool",
    )(comp)
    message = pl.pallas_call(
        pack_kernel,
        out_shape=jax.ShapeDtypeStruct((32, LANES), jnp.float32),
        in_specs=[VMEM] * 2,
        out_specs=VMEM,
        cost_estimate=pl.CostEstimate(flops=10_000, bytes_accessed=40_000, transcendentals=0),
        compiler_params=PARAMS,
        name="pack",
    )(source, guess)
    return message, first, second


def beside_in_plane(v):
    rows, lanes = rows_of(v.shape), lanes_of(v.shape)
    last_row, last_lane = v.shape[0] - 1, v.shape[1] - 1
    total = jnp.where(rows == 0, 0.0, pltpu.roll(v, 1, 0))
    total = total + jnp.where(rows == last_row, 0.0, pltpu.roll(v, last_row, 0))
    total = total + jnp.where(lanes == 0, 0.0, pltpu.roll(v, 1, 1))
    return total + jnp.where(lanes == last_lane, 0.0, pltpu.roll(v, last_lane, 1))


def chem_of(below, c, above):
    beside = beside_in_plane(c) + below + above
    return c * c * c - c - gradient_energy * (beside - 6.0 * c)


def stepped(c, below, v, above):
    beside = beside_in_plane(v) + below + above
    return c + time_step * (beside - 6.0 * v)


def inner_kernel(comp_ref, base_ref, chem_ref):
    planes = comp_ref.shape[0]

    def plane(ref, f):
        return ref[f] if 0 <= f < planes else 0.0

    for f in range(planes):
        chem_ref[f] = chem_of(plane(comp_ref, f - 1), comp_ref[f], plane(comp_ref, f + 1))
    for f in range(planes):
        base_ref[f] = stepped(
            comp_ref[f], plane(chem_ref, f - 1), chem_ref[f], plane(chem_ref, f + 1)
        )


def inner_of(comp):
    return pl.pallas_call(
        inner_kernel,
        out_shape=jax.ShapeDtypeStruct(comp.shape, jnp.float32),
        in_specs=[VMEM],
        out_specs=VMEM,
        scratch_shapes=[pltpu.VMEM(comp.shape, jnp.float32)],
        cost_estimate=pl.CostEstimate(flops=5_000_000, bytes_accessed=1_500_000, transcendentals=0),
        compiler_params=PARAMS,
        name="inner",
    )(comp)


def outer_kernel(comp_ref, first_ref, second_ref, inner_ref, base_ref):
    planes = comp_ref.shape[0]
    group, groups = lax.axis_index("grp"), lax.axis_size("grp")
    index = lax.axis_index("slab") * groups + group
    devices = lax.axis_size("slab") * groups
    odd = lax.rem(group, 2) == 1
    below = jnp.where(index > 0, 1.0, 0.0)
    above = jnp.where(index < devices - 1, 1.0, 0.0)
    sides = (
        (0, 1, below, first_ref, second_ref, 1, 0),
        (planes - 1, planes - 2, above, second_ref, first_ref, 0, 1),
    )
    for side, (edge, next_in, there, if_odd, if_even, near, far) in enumerate(sides):
        beyond = jnp.where(odd, if_odd[near], if_even[near]) * there
        further = jnp.where(odd, if_odd[far], if_even[far]) * there
        around = further + there * comp_ref[edge] + 2.0 * beside_in_plane(beyond) - 12.0 * beyond
        gain = beyond * beyond * beyond - beyond - gradient_energy * around
        base_ref[3 * side] = inner_ref[edge] + time_step * gain
        base_ref[1 + side] = inner_ref[next_in] - time_step * gradient_energy * beyond


def outer_of(comp, first, second, inner):
    return pl.pallas_call(
        outer_kernel,
        out_shape=jax.ShapeDtypeStruct((4,) + comp.shape[1:], jnp.float32),
        in_specs=[VMEM] * 4,
        out_specs=VMEM,
        cost_estimate=pl.CostEstimate(flops=1_000_000, bytes_accessed=1_000_000, transcendentals=0),
        compiler_params=PARAMS,
        name="outer",
    )(comp, first, second, inner)


def rolled(v, step):
    on = [pltpu.roll(here, LANES - 32 * step, 1) for here in v]
    back = on if 64 * step == LANES else [pltpu.roll(here, 32 * step, 1) for here in v]
    return on, back


def beside(v, quad, step, turned):
    here = v[quad]
    on, back = turned
    rows, lanes = rows_of(here.shape), lanes_of(here.shape)
    columns = lanes % 32
    next_quad = on[quad + 1] if quad + 1 < len(v) else 0.0
    last_quad = back[quad - 1] if quad else 0.0
    total = jnp.where(lanes < LANES - 32 * step, on[quad], next_quad)
    total = total + jnp.where(lanes >= 32 * step, back[quad], last_quad)
    total = total + jnp.where(rows < step, 0.0, pltpu.roll(here, step, 0))
    total = total + jnp.where(rows >= 32 - step, 0.0, pltpu.roll(here, 32 - step, 0))
    total = total + jnp.where(columns < step, 0.0, pltpu.roll(here, step, 1))
    return total + jnp.where(columns >= 32 - step, 0.0, pltpu.roll(here, LANES - step, 1))


def operated(v):
    turned = rolled(v, 1)
    return [
        screening * here - (beside(v, quad, 1, turned) - 6.0 * here) for quad, here in enumerate(v)
    ]


def pair_sum(v, step, axis):
    index = (rows_of(v.shape), lanes_of(v.shape))[axis] // step
    other = v.shape[axis] - step
    return v + jnp.where(index % 2 == 0, pltpu.roll(v, other, axis), pltpu.roll(v, step, axis))


def square_sum(v):
    return pair_sum(pair_sum(v, 1, 1), 1, 0)


def cell_mean(v):
    return square_sum(pair_sum(v, 32, 1)) * 0.125


def in_plane(v):
    rows, columns = rows_of(v.shape), lanes_of(v.shape) % 32
    total = jnp.where(rows == 0, 0.0, pltpu.roll(v, 1, 0))
    total = total + jnp.where(rows == 31, 0.0, pltpu.roll(v, 31, 0))
    total = total + jnp.where(columns == 0, 0.0, pltpu.roll(v, 1, 1))
    return total + jnp.where(columns == 31, 0.0, pltpu.roll(v, LANES - 1, 1))


def source_of(even, uneven):
    low_half = lanes_of((16, LANES)) < 64
    top = jnp.where(low_half, even, pltpu.roll(uneven, 64, 1))
    bottom = jnp.where(low_half, pltpu.roll(even, 64, 1), uneven)
    return jnp.concatenate([top, bottom], axis=0)


def widen():
    square = (LANES, LANES)
    return jnp.where(rows_of(square) == lanes_of(square) // 4, 1.0, 0.0).astype(jnp.float32)


scale = damping / (screening + 6.0)
scale_b = damping / (screening + 1.5)
factor = time_step * long_range
edge_share = 0.125 * scale_b * (0.25 * scale_b) ** 2 * scale**2 * factor


def edge_kernel(own_ref, edge_ref, guess_s):
    groups, group = lax.axis_size("grp"), lax.axis_index("grp")
    quads, block = groups // 2, 32 // groups
    up = group == groups - 1
    at = 16 + jnp.where(up, (quads - 1) * block, 0)
    for g in range(groups):
        guess_s[g * block : (g + 1) * block] = own_ref[g, pl.ds(pl.multiple_of(at, block), block)]
    guess = guess_s[...]
    source = jnp.where(
        up,
        source_of(own_ref[groups - 2, 0:16], own_ref[groups - 1, 0:16]),
        source_of(own_ref[0, 0:16], own_ref[1, 0:16]),
    )
    inner = jnp.where(up, pltpu.roll(guess, 32, 1), pltpu.roll(guess, LANES - 32, 1))
    flat = in_plane(guess)
    pre = guess + scale * (source - (screening * guess - (flat + inner - 6.0 * guess)))
    value = square_sum(pre + scale * (flat - (screening + 5.0) * guess))
    value = jnp.where(up, pltpu.roll(value, 32, 1), value)
    edge_ref[...] = edge_share * exact_dot(value, widen())


def edge_of(own):
    return pl.pallas_call(
        edge_kernel,
        out_shape=jax.ShapeDtypeStruct((32, LANES), jnp.float32),
        in_specs=[VMEM],
        out_specs=VMEM,
        scratch_shapes=[pltpu.VMEM((32, LANES), jnp.float32)],
        cost_estimate=pl.CostEstimate(flops=500_000, bytes_accessed=80_000, transcendentals=0),
        compiler_params=PARAMS,
        name="edge",
    )(own)


def solve_kernel(edged, own_ref, core_ref, chip_ref, wide_ref, rows_ref, guess_s, window_s):
    groups = lax.axis_size("grp")
    slab, slabs, group = lax.axis_index("slab"), lax.axis_size("slab"), lax.axis_index("grp")
    quads = groups // 2
    block = 32 // groups
    odd = lax.rem(slab, 2) == 1

    def low(*at):
        return jnp.where(odd, core_ref[at], chip_ref[at])

    def high(*at):
        return jnp.where(odd, chip_ref[at], core_ref[at])

    def own(*at):
        return own_ref[at]

    source = []

    def take(read, quad):
        at = len(source)
        source.append(source_of(read(2 * quad, pl.ds(0, 16)), read(2 * quad + 1, pl.ds(0, 16))))
        for g in range(groups):
            guess_s[at, g * block : (g + 1) * block] = read(g, pl.ds(16 + quad * block, block))

    near, trim = (quads, 0) if edged else (HALO, 1)
    for quad in range(quads - near, quads):
        take(low, quad)
    for quad in range(quads):
        take(own, quad)
    for quad in range(near):
        take(high, quad)
    total = quads + 2 * near
    has_low = jnp.where(slab > 0, 1.0, 0.0)
    has_high = jnp.where(slab < slabs - 1, 1.0, 0.0)

    def kept(v, quad):
        if quad < near:
            return v * has_low
        return v if quad < near + quads else v * has_high

    guess = [kept(guess_s[quad], quad) for quad in range(total)]
    applied = operated(guess)
    pre = [
        kept(guess[quad] + scale * (source[quad] - applied[quad]), quad) for quad in range(total)
    ]
    applied = operated(pre)
    coarsest = [
        kept(cell_mean(source[quad] - applied[quad]), quad) for quad in range(trim, total - trim)
    ]
    correction = [scale_b * v for v in coarsest]
    for sweep in range(NCOARSE - 1):
        last = sweep == NCOARSE - 2
        updated = []
        turned = rolled(correction, 2)
        for quad in range(len(correction)):
            if last and quad in (0, len(correction) - 1):
                updated.append(None)
                continue
            c = correction[quad]
            applied = screening * c - 0.25 * (beside(correction, quad, 2, turned) - 6.0 * c)
            updated.append(kept(c + scale_b * (coarsest[quad] - applied), quad + trim))
        correction = updated
    start = near - 1
    found = [pre[quad] + correction[quad - trim] for quad in range(start, total - start)]
    for _ in range(NPOST):
        applied = operated(found)
        found = [
            kept(v + scale * (source[quad + start] - applied[quad]), quad + start)
            for quad, v in enumerate(found)
        ]

    for quad in range(len(found)):
        window_s[quad] = found[quad]
    for quad in range(quads):
        rows_ref[quad] = window_s[quad + 1, pl.ds(pl.multiple_of(group * block, block), block), :]

    picked = []
    for i in range(4):
        at = 2 * group + 3 + i
        picked.append(
            pltpu.roll(window_s[at // QUAD], lax.rem(LANES - 32 * lax.rem(at, QUAD), LANES), 1)
        )
    if edged:
        lowest = group == 0
        facing = jnp.where(lowest, guess[0], pltpu.roll(guess[total - 1], 32, 1))
        reach = jnp.where(lowest, slab, slabs - 1 - slab) >= 2
        picked.append(jnp.where(reach, edge_share * scale / factor, 0.0) * square_sum(facing))
    wide = factor * exact_dot(jnp.concatenate(picked, axis=0), widen())
    wide = [wide[32 * i : 32 * (i + 1)] for i in range(len(picked))]
    if edged:
        wide[0] = wide[0] + jnp.where(group == 0, 1.0, 0.0) * wide[4]
        wide[3] = wide[3] + jnp.where(group == groups - 1, 1.0, 0.0) * wide[4]
    for i in range(4):
        wide_ref[i] = wide[i]


def solve(own, core, chip, guess, edged):
    groups = own.shape[0]
    quads = groups // 2
    total = 3 * quads if edged else quads + 2 * HALO
    return pl.pallas_call(
        functools.partial(solve_kernel, edged),
        out_shape=(
            jax.ShapeDtypeStruct((4, 32, LANES), jnp.float32),
            jax.ShapeDtypeStruct((quads, guess.shape[1], LANES), jnp.float32),
        ),
        in_specs=[VMEM] * 3,
        out_specs=(VMEM, VMEM),
        scratch_shapes=[
            pltpu.VMEM((total, 32, LANES), jnp.float32),
            pltpu.VMEM((quads + 2, 32, LANES), jnp.float32),
        ],
        cost_estimate=pl.CostEstimate(flops=6_000_000, bytes_accessed=500_000, transcendentals=0),
        compiler_params=PARAMS,
        name="solve",
    )(own, core, chip)


def finish_kernel(inner_ref, outer_ref, wide_ref, rows_ref, *refs):
    edge_ref = refs[0] if len(refs) == 3 else None
    next_ref, potential_ref = refs[-2:]
    group, groups = lax.axis_index("grp"), lax.axis_size("grp")
    slab, slabs = lax.axis_index("slab"), lax.axis_size("slab")
    for quad in range(rows_ref.shape[0]):
        for i in range(QUAD):
            potential_ref[QUAD * quad + i] = rows_ref[quad, :, 32 * i : 32 * (i + 1)]
    wide = [wide_ref[i] for i in range(4)]
    if edge_ref is not None:
        lowest = (group == 0) & (slab >= 2)
        highest = (group == groups - 1) & (slab < slabs - 2)
        wide[0] = wide[0] + jnp.where(lowest, 1.0, 0.0) * edge_ref[...]
        wide[3] = wide[3] + jnp.where(highest, 1.0, 0.0) * edge_ref[...]
    rows, lanes = rows_of((32, LANES)), lanes_of((32, LANES))
    for coarse in range(2):
        here = wide[coarse + 1]
        across = jnp.where(lanes == 0, 0.0, pltpu.roll(here, 1, 1))
        across = across + jnp.where(lanes == LANES - 1, 0.0, pltpu.roll(here, LANES - 1, 1))
        middle = across - 2.0 * here
        before = middle + (jnp.where(rows == 0, 0.0, pltpu.roll(here, 1, 0)) - here)
        after = middle + (jnp.where(rows == 31, 0.0, pltpu.roll(here, 31, 0)) - here)
        down = wide[coarse] - here
        up = wide[coarse + 2] - here
        for f in range(4):
            for j in range(4):
                term = (before, middle, middle, after)[j]
                if f == 0:
                    term = term + down
                if f == 3:
                    term = term + up
                plane, within = 4 * coarse + f, (pl.ds(j, 32, stride=4), slice(None))
                if 2 <= plane < 6:
                    base = inner_ref[(plane, *within)]
                else:
                    base = outer_ref[(plane % 4, *within)]
                next_ref[(plane, *within)] = base + term


def finish(inner, outer, wide, rows, edge, guess):
    operands = [inner, outer, wide, rows] + ([] if edge is None else [edge])
    return pl.pallas_call(
        finish_kernel,
        out_shape=(
            jax.ShapeDtypeStruct(inner.shape, jnp.float32),
            jax.ShapeDtypeStruct(guess.shape, jnp.float32),
        ),
        in_specs=[VMEM] * len(operands),
        out_specs=(VMEM, VMEM),
        cost_estimate=pl.CostEstimate(flops=500_000, bytes_accessed=1_100_000, transcendentals=0),
        compiler_params=PARAMS,
        name="finish",
    )(*operands)


def pairing(*pairs):
    return [p for a, b in pairs for p in {(a, b), (b, a)}]


def per_device(comp, guess):
    slabs, groups = lax.axis_size("slab"), lax.axis_size("grp")
    group = lax.axis_index("grp")
    both = ("slab", "grp")
    devices = slabs * groups
    quads = groups // 2

    def at(slab, member):
        return slab * groups + member

    message, first, second = pack(comp, guess)


    bundle = jnp.broadcast_to(message, (groups,) + message.shape)
    for k in range(1, groups):
        block = lax.ppermute(message, "grp", [(i, i ^ k) for i in range(groups)])
        bundle = lax.dynamic_update_slice(bundle, block[None], (group ^ k, 0, 0))

    first = lax.ppermute(first, both, pairing(*((d, d + 1) for d in range(0, devices, 2))))
    second = lax.ppermute(
        second,
        both,
        pairing(
            *((d, d + 1) for d in range(1, devices - 1, 2)), *idle_second(devices)
        ),
    )

    core = lax.ppermute(bundle, "slab", pairing(*((i, i + 1) for i in range(0, slabs, 2))))
    chip = lax.ppermute(
        bundle,
        both,
        pairing(
            *((at(i, g), at(i + 1, g)) for i in range(1, slabs - 1, 2) for g in range(groups)),
            *idle_chip(at, slabs, groups),
        ),
    )
    edge = None
    if quads < HALO:
        edge = lax.ppermute(edge_of(bundle), both, edge_pairs(at, slabs, groups))

    inner = inner_of(comp)
    wide, rows = solve(bundle, core, chip, guess, edge is not None)
    outer = outer_of(comp, first, second, inner)
    return finish(inner, outer, wide, rows, edge, guess)


def idle_second(devices):
    return [(0, 0), (devices - 1, devices - 1)]


def idle_chip(at, slabs, groups):
    half = groups // 2
    return [(at(s, g), at(s, g + half)) for s in (0, slabs - 1) for g in range(half)]


def edge_pairs(at, slabs, groups):
    top = groups - 1
    return pairing(
        *((at(i, top), at(i + 2, 0)) for i in range(slabs - 2)),
        *((at(i, g), at(i + 1, g)) for i in range(0, slabs, 2) for g in range(1, top)),
        (at(0, 0), at(1, 0)),
        (at(slabs - 2, top), at(slabs - 1, top)),
    )


def solution(mesh):
    placed = (P(("slab", "grp"), None, None), P("slab", "grp", None))
    return jax.shard_map(per_device, mesh=mesh, in_specs=placed, out_specs=placed, check_vma=False)
```
